32 devices in a mesh: band: 8 (over z, x), dir: 4 (over y, core).
Axes of the slice: x: 2, y: 2, z: 4, core: 2. Of those that a mesh axis runs over, the one named last changes fastest.
Arguments:
- visibilities: bfloat16 [16, 32, 2, 256, 256], P('band', 'dir'), as said below
- sky_model: bfloat16 [16, 32, 2, 256, 256], P('band', 'dir')
- rfi_flags: int32 [16, 8, 8], P('band'), may hold values from 0 to 1, as said below
- destination: int32 [16], P('band'), may hold values from 0 to 15, as said below
Outputs:
- delivered: float32 [16, 32, 2, 256], P('band', 'dir')
- coefficients: float32 [9, 32, 2, 256], P(None, 'dir')
- norm_values: float32 [2, 2], replicated
The draws below stay inside these ranges and needn't reach their ends.
Inputs may be any that keep to these rules, and one draw needn't show every extreme that they name: `rfi_flags`: 1 marks a flagged baseline block; the share of flagged blocks tends to fall with the subband index. destination holds every row of 0 to 15 once. With the rows split into 8 aligned blocks of 2 rows, one row of block i goes to a row of block i + 1 and the other to a row of block i + 4, modulo 16 // 2. `visibilities`: visibilities follow the model under unknown station gains, with noise.
All inputs are finite; a program needn't handle non-finite values.
Results may differ from the reference program's by a relative error of at most 0.0003.
Values sent between devices are 32-bit elements; how exact they have to be, the bound alone decides.
No kernel may reach another device: no remote copies, remote signals or barrier semaphores. Data moves between devices by JAX's collectives and lax.ppermute only.
A program may use at most 128 MiB of HBM per device.

```python
import jax
import jax.numpy as jnp
from jax import lax

STATIONS = 256
DIRECTIONS = 32
BLOCK = 32
DEGREE = 8
SWEEPS = 4
ITERS = 2
SB_DEV = 2
SUBBANDS = 16


def band_pair(key, band_row):
    band_key = jax.random.fold_in(jax.random.fold_in(key, 11), band_row)
    model_key, noise_key, rough_key = jax.random.split(band_key, 3)
    shared = jax.random.normal(jax.random.fold_in(key, 23), (4, DIRECTIONS, STATIONS), jnp.float32)
    rough = jax.random.normal(rough_key, (2, DIRECTIONS, STATIONS), jnp.float32)
    abscissa = (2.0 * band_row.astype(jnp.float32) + 1.0) / SUBBANDS - 1.0
    sky_values = jax.random.normal(model_key, (DIRECTIONS, 2, STATIONS, STATIONS), jnp.float32)
    noise_level = 0.5
    amp_spread = 0.25
    amplitude = 1.0 + amp_spread * shared[0] + 0.15 * abscissa * shared[1] + 0.1 * rough[0]
    phase = 0.8 * shared[2] + 0.5 * abscissa * shared[3] + 0.2 * rough[1]
    gain_re = amplitude * jnp.cos(phase)
    gain_im = amplitude * jnp.sin(phase)
    model_re = sky_values[:, 0]
    model_im = sky_values[:, 1]
    twist_re = model_re * gain_re[:, None, :] + model_im * gain_im[:, None, :]
    twist_im = model_im * gain_re[:, None, :] - model_re * gain_im[:, None, :]
    noise = jax.random.normal(noise_key, (2, DIRECTIONS, STATIONS, STATIONS), jnp.float32)
    data_re = gain_re[:, :, None] * twist_re - gain_im[:, :, None] * twist_im + noise_level * noise[0]
    data_im = gain_re[:, :, None] * twist_im + gain_im[:, :, None] * twist_re + noise_level * noise[1]
    return (sky_values.astype(jnp.bfloat16), jnp.stack([data_re, data_im], axis=1).astype(jnp.bfloat16))


def draw_sky_model(key, part):

    def one_band(band_row):
        return band_pair(key, band_row)[0]
    return lax.map(one_band, jnp.arange(SUBBANDS))


def draw_visibilities(key, part):

    def one_band(band_row):
        return band_pair(key, band_row)[1]
    return lax.map(one_band, jnp.arange(SUBBANDS))


def draw_rfi_flags(key, part):
    band_rows = jnp.arange(SUBBANDS)
    threshold = 750 - 600 * band_rows // max(SUBBANDS - 1, 1)
    blocks = STATIONS // BLOCK
    random_ints = jax.random.randint(jax.random.fold_in(key, 5), (SUBBANDS, blocks, blocks), 0, 1000)
    return (random_ints < threshold[:, None, None]).astype(jnp.int32)


def draw_destination(key, part):
    block_count = SUBBANDS // SB_DEV
    half_count = block_count // 2
    base_key = jax.random.fold_in(key, 7)
    send_key, recv_key = jax.random.split(base_key)
    send_perm = jax.vmap(lambda one_key: jax.random.permutation(one_key, SB_DEV))(jax.random.split(send_key, block_count))
    recv_perm = jax.vmap(lambda one_key: jax.random.permutation(one_key, SB_DEV))(jax.random.split(recv_key, block_count))
    block_ids = jnp.arange(block_count)[:, None]
    slot_ids = jnp.arange(SB_DEV)[None, :]
    source_rows = block_ids * SB_DEV + send_perm
    target_block = jnp.where(slot_ids == 0, (block_ids + 1) % block_count, jnp.where(slot_ids == 1, (block_ids + half_count) % block_count, block_ids + 0 * slot_ids))
    target_slot = recv_perm[target_block, slot_ids + 0 * block_ids]
    target_rows = target_block * SB_DEV + target_slot
    result = jnp.zeros((SUBBANDS,), jnp.int32).at[source_rows.reshape(-1)].set(target_rows.reshape(-1).astype(jnp.int32))
    return result.astype(jnp.int32)


def setup_inputs(seed: int = 0) -> dict:
    streams_of = jax.random.split(jax.random.key(seed), 5)
    return {
        "visibilities": draw_visibilities(jax.random.fold_in(streams_of[4], 71), 0),
        "sky_model": draw_sky_model(jax.random.fold_in(streams_of[4], 71), 0),
        "rfi_flags": draw_rfi_flags(jax.random.fold_in(streams_of[4], 71), 0),
        "destination": draw_destination(jax.random.fold_in(streams_of[4], 71), 0),
    }


highest = lax.Precision.HIGHEST
penalty_share = 0.4

def block_weights(rfi_flags):
    blocks = rfi_flags.shape[-1]
    kept_blocks = (1 - rfi_flags).astype(jnp.float32)
    leading = kept_blocks.shape[:-2]
    spread = jnp.broadcast_to(kept_blocks[..., :, None, :, None], leading + (blocks, BLOCK, blocks, BLOCK))
    stations = blocks * BLOCK
    spread = spread.reshape(leading + (stations, stations))
    return spread * (1.0 - jnp.eye(stations, dtype=jnp.float32))

def operators(visibilities, sky_model, rfi_flags):
    baseline = block_weights(rfi_flags)[..., None, :, :]
    data_re = visibilities[..., 0, :, :].astype(jnp.float32)
    data_im = visibilities[..., 1, :, :].astype(jnp.float32)
    model_re = sky_model[..., 0, :, :].astype(jnp.float32)
    model_im = sky_model[..., 1, :, :].astype(jnp.float32)
    oper_re = baseline * (model_re * data_re + model_im * data_im)
    oper_im = baseline * (model_re * data_im - model_im * data_re)
    square = baseline * (model_re * model_re + model_im * model_im)
    return (jnp.stack([oper_re, oper_im], axis=-3), square)

def chebyshev(band_rows, band_total):
    abscissa = (2.0 * band_rows + 1.0) / band_total - 1.0
    cheb_terms = [jnp.ones_like(abscissa), abscissa]
    for degree in range(2, DEGREE + 1):
        cheb_terms.append(2.0 * abscissa * cheb_terms[-1] - cheb_terms[-2])
    return jnp.stack(cheb_terms[:DEGREE + 1], axis=0)

def stefcal(operator, square, gain_now, target, penalty):
    pen_term = penalty[..., None, None, None]
    for sweep_index in range(SWEEPS):
        products = jnp.einsum('...kapq,...kbq->...kabp', operator, gain_now, precision=highest)
        real_part = products[..., 0, 0, :] - products[..., 1, 1, :]
        imag_part = products[..., 0, 1, :] + products[..., 1, 0, :]
        numerator = jnp.stack([real_part, imag_part], axis=-2)
        magnitude = lax.optimization_barrier(jnp.sum(gain_now * gain_now, axis=-2))
        denominator = jnp.einsum('...kpq,...kq->...kp', square, magnitude, precision=highest)
        updated = (numerator + pen_term * target) / (denominator[..., None, :] + pen_term)
        gain_now = 0.5 * (updated + gain_now) if sweep_index % 2 == 1 else updated
    return gain_now

def per_band(band_items):
    vis_band, model_band, flag_band, gain_band, target_band, pen_band = band_items
    operator, square = operators(vis_band, model_band, flag_band)
    return stefcal(operator, square, gain_band, target_band, pen_band)

def reference(visibilities, sky_model, rfi_flags, destination):
    band_total = visibilities.shape[0]
    directions = visibilities.shape[1]
    stations = visibilities.shape[-1]
    blocks = rfi_flags.shape[-1]
    weights = (1.0 + lax.optimization_barrier(jnp.sum(1 - rfi_flags, axis=(1, 2))).astype(jnp.float32)) / (1.0 + blocks * blocks)
    penalty = penalty_share * stations * weights
    cheb_basis = chebyshev(jnp.arange(band_total).astype(jnp.float32), band_total)
    weighted = cheb_basis * weights[None, :]
    gram_matrix = jnp.dot(weighted, cheb_basis.T, precision=highest)
    factor = jnp.linalg.cholesky(gram_matrix)
    normalizer = directions * 2.0 * stations * gram_matrix[0, 0]
    ones_part = jnp.ones((band_total, directions, stations), jnp.float32)
    unit_gains = jnp.stack([ones_part, jnp.zeros_like(ones_part)], axis=2)
    gain_now = unit_gains
    consensus = unit_gains
    dual_var = jnp.zeros_like(unit_gains)
    row_weight = weights[:, None, None, None]
    norm_rows = []
    coefficients = None
    for iteration in range(ITERS):
        gain_now = lax.map(per_band, (visibilities, sky_model, rfi_flags, gain_now, consensus - dual_var, penalty))
        projection = jnp.einsum('cs,skap->ckap', weighted, gain_now + dual_var, precision=highest)
        flat_proj = projection.reshape(projection.shape[0], -1)
        coefficients = jax.scipy.linalg.cho_solve((factor, True), flat_proj).reshape(projection.shape)
        fresh_gains = jnp.einsum('cs,ckap->skap', cheb_basis, coefficients, precision=highest)
        dual_var = dual_var + gain_now - fresh_gains
        primal = jnp.sqrt(jnp.sum(row_weight * (gain_now - fresh_gains) ** 2) / normalizer)
        dual_norm = jnp.sqrt(jnp.sum(row_weight * (fresh_gains - consensus) ** 2) / normalizer)
        norm_rows.append(jnp.stack([primal, dual_norm]))
        consensus = fresh_gains
    delivered = jnp.zeros_like(gain_now).at[destination].set(gain_now)
    return (delivered, coefficients, jnp.stack(norm_rows))
```

```python
import functools

import jax
import jax.numpy as jnp
from jax import lax
from jax.experimental import pallas as pl
from jax.experimental.pallas import tpu as pltpu
from jax.sharding import PartitionSpec as P

DEGREE = 8
SWEEPS = 4
ITERS = 2
PENALTY_SHARE = 0.4
LANES = 128
SUBLANES = 8

highest = lax.Precision.HIGHEST
f32 = jnp.float32
bf16 = jnp.bfloat16


def round_up(value, step):
    return -(-value // step) * step


def roll_rows(x, shift):
    return pltpu.roll(x, shift % x.shape[0], 0)


def row_pattern(stations):
    rows = lax.broadcasted_iota(jnp.int32, (SUBLANES, stations), 0)
    even = rows % 2 == 0
    first = rows % 4 < 2
    return even, first


def split_rows(x, even):
    high = x.astype(bf16).astype(f32)
    return jnp.where(even, high, x - high)


def add_pairs(x, even):
    return x + jnp.where(even, roll_rows(x, -1), roll_rows(x, 1))


def sweep(load_oper, gain, target_term, pen, average, even, first):
    stations = gain.shape[1]
    halves = split_rows(gain, even)
    crossed = roll_rows(halves, 2)
    crossed = jnp.where(first, -crossed, crossed)
    square = gain * gain
    magnitude = split_rows(square + roll_rows(square, 2), even)
    halves, crossed, magnitude = [v.astype(bf16) for v in (halves, crossed, magnitude)]
    lhs = jnp.concatenate([halves, halves, crossed, crossed], axis=1)
    numerator = jnp.dot(lhs, load_oper(0, 4 * stations), preferred_element_type=f32)
    lhs = jnp.concatenate([magnitude, magnitude], axis=1)
    denominator = jnp.dot(
        lhs, load_oper(4 * stations, 2 * stations), preferred_element_type=f32
    )
    numerator = add_pairs(numerator, even)
    denominator = add_pairs(denominator, even)
    updated = (numerator + target_term) / (denominator + pen)
    return 0.5 * (updated + gain) if average else updated


def to_rows(real, imag, first):
    return jnp.where(first, real, imag)


def band_weight(flags_ref, f, blocks):
    flagged = jnp.int32(0)
    for i in range(blocks):
        for j in range(blocks):
            flagged = flagged + flags_ref[f, i, j]
    kept = (blocks * blocks - flagged).astype(f32)
    return (1.0 + kept) / (1.0 + blocks * blocks)


def first_kernel(
    flags_ref, dest_ref, vis_ref, sky_ref, oper_ref, gain_ref, mask_ref, turned_ref
):
    step = pl.program_id(0)
    bands, group, _, stations, _ = vis_ref.shape
    blocks = flags_ref.shape[-1]
    block = stations // blocks
    lanes = gain_ref.shape[1] - LANES
    even, first = row_pattern(stations)

    @pl.when(step == 0)
    def _():
        cols = lax.broadcasted_iota(jnp.int32, (block, stations), 1)
        rows = lax.broadcasted_iota(jnp.int32, (block, stations), 0)
        for f in range(bands):
            for i in range(blocks):
                keep = jnp.zeros((block, stations), f32)
                for j in range(blocks):
                    value = (1 - flags_ref[f, i, j]).astype(f32)
                    keep = jnp.where(cols // block == j, value, keep)
                keep = jnp.where(cols == rows + i * block, 0.0, keep)
                mask_ref[f, pl.ds(i * block, block), :] = keep.astype(bf16)
            weight = band_weight(flags_ref, f, blocks)
            lane = lax.broadcasted_iota(jnp.int32, (1, LANES), 1)
            extra = jnp.where(lane == 0, weight, dest_ref[f].astype(f32))
            gain_ref[pl.ds(f, 1), pl.ds(lanes, LANES)] = extra

    chunk = 32
    gains = []
    penalties = []
    for f in range(bands):
        weight = band_weight(flags_ref, f, blocks)
        pen = PENALTY_SHARE * stations * weight
        for k in range(group):
            pair = (step * group + k) * bands + f
            mask = mask_ref[f]
            for a in range(2):
                turned_ref[a] = (sky_ref[f, k, a] * mask).T
                turned_ref[2 + a] = vis_ref[f, k, a].T
            totals = [jnp.zeros((SUBLANES, stations), f32) for _ in range(3)]
            for c in range(stations // chunk):
                part = pl.ds(c * chunk, chunk)
                model_re, model_im, data_re, data_im = [
                    turned_ref[a, part, :].astype(f32) for a in range(4)
                ]
                values = (
                    model_re * data_re + model_im * data_im,
                    model_re * data_im - model_im * data_re,
                    model_re * model_re + model_im * model_im,
                )
                for n, value in enumerate(values):
                    high = value.astype(bf16)
                    low = (value - high.astype(f32)).astype(bf16)
                    start = 2 * n * stations + c * chunk
                    oper_ref[pair, pl.ds(start, chunk), :] = high
                    oper_ref[pair, pl.ds(start + stations, chunk), :] = low
                    for r in range(chunk // SUBLANES):
                        totals[n] = totals[n] + value[r * SUBLANES : (r + 1) * SUBLANES]
            sums = [jnp.sum(t, axis=0, keepdims=True) for t in totals]
            scale = sums[2] + pen
            real = (sums[0] + pen) / scale
            imag = sums[1] / scale
            gains.append(to_rows(real, imag, first))
            penalties.append(pen)
    for index in range(1, SWEEPS):
        number = 0
        for f in range(bands):
            for k in range(group):
                pair = (step * group + k) * bands + f
                pen = penalties[number]

                def load_oper(start, size, pair=pair):
                    return oper_ref[pair, pl.ds(start, size), :]

                target_term = jnp.where(first, pen, 0.0)
                gains[number] = sweep(
                    load_oper, gains[number], target_term, pen, index % 2 == 1, even, first
                )
                number += 1
    number = 0
    for f in range(bands):
        for k in range(group):
            for a in range(2):
                start = pl.multiple_of(((step * group + k) * 2 + a) * stations, stations)
                gain_ref[pl.ds(f, 1), pl.ds(start, stations)] = gains[number][
                    2 * a : 2 * a + 1
                ]
            number += 1


def chebyshev_columns(abscissa, width):
    lane = lax.broadcasted_iota(jnp.int32, (abscissa.shape[0], width), 1)
    terms = [jnp.ones_like(abscissa), abscissa]
    for degree in range(2, DEGREE + 1):
        terms.append(2.0 * abscissa * terms[-1] - terms[-2])
    basis = jnp.zeros((abscissa.shape[0], width), f32)
    for degree in range(DEGREE + 1):
        basis = jnp.where(lane == degree, terms[degree], basis)
    return basis


def fit_matrix(basis, weight):
    rows, width = basis.shape
    terms = round_up(DEGREE + 1, SUBLANES)
    span = round_up(rows, LANES)
    lane = lax.broadcasted_iota(jnp.int32, (rows, span), 1)
    row = lax.broadcasted_iota(jnp.int32, (rows, span), 0)
    identity = jnp.where(lane == row, 1.0, 0.0)
    weighted = basis * weight
    right = jnp.concatenate([basis, identity], axis=1)
    system = lax.dot_general(
        weighted, right, (((0,), (0,)), ((), ())), precision=highest,
        preferred_element_type=f32,
    )[:terms]
    line = lax.broadcasted_iota(jnp.int32, system.shape, 0)
    for j in range(DEGREE + 1):
        pivot = system[j : j + 1] / system[j : j + 1, j : j + 1]
        system = jnp.where(line == j, pivot, system - system[:, j : j + 1] * pivot)
    return system[:, width : width + rows], system[0:1, 0:1]


def second_kernel(
    index_ref, flags_ref, all_ref, oper_ref, gain_ref, fresh_ref, dual_ref, fit_ref
):
    bands = gain_ref.shape[0]
    lanes = gain_ref.shape[1]
    rows = all_ref.shape[0]
    blocks = flags_ref.shape[-1]
    pairs = oper_ref.shape[0]
    stations = oper_ref.shape[2]
    even, first = row_pattern(stations)
    basis = gathered_basis(index_ref[0], bands, rows)
    weight = all_ref[:, pl.ds(lanes, 1)]
    fit, _ = fit_matrix(basis, weight)
    fit_ref[...] = jnp.zeros_like(fit_ref)
    fit_ref[:, pl.ds(0, rows)] = fit
    project = jnp.dot(
        basis[:, : fit.shape[0]], fit, precision=highest, preferred_element_type=f32
    )
    own = all_ref[:, pl.ds(0, lanes)]
    fresh = jnp.dot(project, own, precision=highest, preferred_element_type=f32)
    fresh_ref[...] = fresh
    dual_ref[...] = own - fresh
    group = 4
    for start in range(0, pairs, group):
        gains = []
        targets = []
        penalties = []
        for pair in range(start, start + group):
            k, f = divmod(pair, bands)
            pen = PENALTY_SHARE * stations * band_weight(flags_ref, f, blocks)
            parts = [pl.ds((2 * k + a) * stations, stations) for a in range(2)]
            line = pl.ds(f, 1)
            gains.append(
                to_rows(all_ref[line, parts[0]], all_ref[line, parts[1]], first)
            )
            goal = [fresh_ref[line, p] - dual_ref[line, p] for p in parts]
            targets.append(pen * to_rows(goal[0], goal[1], first))
            penalties.append(pen)
        for index in range(SWEEPS):
            for n in range(group):
                pair = start + n

                def load_oper(begin, size, pair=pair):
                    return oper_ref[pair, pl.ds(begin, size), :]

                gains[n] = sweep(
                    load_oper, gains[n], targets[n], penalties[n], index % 2 == 1, even, first
                )
        for n in range(group):
            k, f = divmod(start + n, bands)
            for a in range(2):
                gain_ref[pl.ds(f, 1), pl.ds((2 * k + a) * stations, stations)] = gains[n][
                    2 * a : 2 * a + 1
                ]


def gathered_basis(index, bands, rows):
    row = lax.broadcasted_iota(jnp.int32, (rows, LANES), 0)
    band_row = ((row // bands) ^ index) * bands + row % bands
    abscissa = (2.0 * band_row.astype(f32) + 1.0) / rows - 1.0
    return chebyshev_columns(abscissa, LANES)


def third_kernel(
    index_ref, last_ref, all_ref, fresh_ref, dual_ref, fit_ref,
    delivered_ref, coefficients_ref, norm_ref,
):
    bands, dirs, _, stations = delivered_ref.shape
    rows, lanes = last_ref.shape
    basis = gathered_basis(index_ref[0], bands, rows)
    weight = all_ref[:, pl.ds(lanes, 1)]
    destination = all_ref[:, pl.ds(lanes + 1, 1)]
    fit = fit_ref[:, pl.ds(0, rows)]
    terms = fit.shape[0]
    gains = last_ref[...]
    dual = dual_ref[...]
    before = fresh_ref[...]
    coefficients = jnp.dot(
        fit, gains + dual, precision=highest, preferred_element_type=f32
    )
    fresh = jnp.dot(
        basis[:, :terms], coefficients, precision=highest, preferred_element_type=f32
    )
    line = lax.broadcasted_iota(jnp.int32, (rows, lanes), 1)
    start = jnp.where((line // stations) % 2 == 0, 1.0, 0.0)
    pieces = [dual * dual, (before - start) ** 2, (gains - fresh) ** 2, (fresh - before) ** 2]
    lane = lax.broadcasted_iota(jnp.int32, (1, LANES), 1)
    norms = jnp.zeros((1, LANES), f32)
    for n, piece in enumerate(pieces):
        norms = jnp.where(lane == n, jnp.sum(piece * weight), norms)
    norms = jnp.where(lane == len(pieces), jnp.sum(weight), norms)
    norm_ref[...] = norms
    for k in range(dirs):
        for a in range(2):
            part = slice((2 * k + a) * stations, (2 * k + a + 1) * stations)
            for c in range(DEGREE + 1):
                coefficients_ref[c, k, pl.ds(a, 1), :] = coefficients[c : c + 1, part]
    for f in range(bands):
        target = (index_ref[0] * bands + f).astype(f32)
        chosen = jnp.sum(jnp.where(destination == target, gains, 0.0), axis=0, keepdims=True)
        for k in range(dirs):
            for a in range(2):
                part = slice((2 * k + a) * stations, (2 * k + a + 1) * stations)
                delivered_ref[f, k, pl.ds(a, 1), :] = chosen[:, part]


def exchange(x, axis, distance):
    size = lax.axis_size(axis)
    return lax.ppermute(x, axis, [(i ^ distance, i) for i in range(size)])


def gather_rows(x, axis):
    size = lax.axis_size(axis)
    distance = 1
    while distance < size:
        x = jnp.concatenate([x, exchange(x, axis, distance)], axis=0)
        distance *= 2
    return x


def add_over(x, axis):
    size = lax.axis_size(axis)
    distance = 1
    while distance < size:
        x = x + exchange(x, axis, distance)
        distance *= 2
    return x


def vmem(*_):
    return pl.BlockSpec(memory_space=pltpu.VMEM)


def smem():
    return pl.BlockSpec(memory_space=pltpu.SMEM)


def per_device(visibilities, sky_model, rfi_flags, destination):
    bands, dirs, _, stations, _ = visibilities.shape
    count = lax.axis_size("band")
    rows = bands * count
    lanes = dirs * 2 * stations
    index = lax.axis_index("band").reshape(1)
    group = 2
    pairs = bands * dirs
    terms = round_up(DEGREE + 1, SUBLANES)
    block = pl.BlockSpec(
        (bands, group, 2, stations, stations), lambda s: (0, s, 0, 0, 0)
    )
    operator, gains = pl.pallas_call(
        first_kernel,
        grid=(dirs // group,),
        out_shape=(
            jax.ShapeDtypeStruct((pairs, 6 * stations, stations), bf16),
            jax.ShapeDtypeStruct((bands, lanes + LANES), f32),
        ),
        in_specs=[smem(), smem(), block, block],
        out_specs=(vmem(), vmem()),
        scratch_shapes=[
            pltpu.VMEM((bands, stations, stations), bf16),
            pltpu.VMEM((4, stations, stations), bf16),
        ],
        compiler_params=pltpu.CompilerParams(
            dimension_semantics=("arbitrary",), vmem_limit_bytes=36 * 2**20
        ),
        name="first",
    )(rfi_flags, destination, visibilities, sky_model)
    everyone = gather_rows(gains, "band")
    gains, fresh, dual, fit = pl.pallas_call(
        second_kernel,
        out_shape=(
            jax.ShapeDtypeStruct((bands, lanes), f32),
            jax.ShapeDtypeStruct((rows, lanes), f32),
            jax.ShapeDtypeStruct((rows, lanes), f32),
            jax.ShapeDtypeStruct((terms, round_up(rows, LANES)), f32),
        ),
        in_specs=[smem(), smem(), vmem(), vmem()],
        out_specs=(vmem(), vmem(), vmem(), vmem()),
        compiler_params=pltpu.CompilerParams(vmem_limit_bytes=36 * 2**20),
        name="second",
    )(index, rfi_flags, everyone, operator)
    last = gather_rows(gains, "band")
    delivered, coefficients, norms = pl.pallas_call(
        third_kernel,
        out_shape=(
            jax.ShapeDtypeStruct((bands, dirs, 2, stations), f32),
            jax.ShapeDtypeStruct((DEGREE + 1, dirs, 2, stations), f32),
            jax.ShapeDtypeStruct((1, LANES), f32),
        ),
        in_specs=[smem()] + [vmem()] * 5,
        out_specs=(vmem(), vmem(), vmem()),
        compiler_params=pltpu.CompilerParams(vmem_limit_bytes=36 * 2**20),
        name="third",
    )(index, last, everyone, fresh, dual, fit)
    scale = lax.axis_size("dir") * dirs * 2.0 * stations
    totals = add_over(norms, "dir")
    weight_sum = norms[0, 2 * ITERS]
    norm_values = jnp.sqrt(totals[0, : 2 * ITERS] / (scale * weight_sum))
    return delivered, coefficients, norm_values.reshape(ITERS, 2)


def solution(mesh):
    return jax.shard_map(
        per_device,
        mesh=mesh,
        in_specs=(
            P("band", "dir", None, None, None),
            P("band", "dir", None, None, None),
            P("band", None, None),
            P("band"),
        ),
        out_specs=(P("band", "dir", None, None), P(None, "dir", None, None), P()),
        check_vma=False,
    )
```

```python
import functools

import jax
import jax.numpy as jnp
from jax import lax
from jax.experimental import pallas as pl
from jax.experimental.pallas import tpu as pltpu
from jax.sharding import PartitionSpec as P

DEGREE = 8
SWEEPS = 4
ITERS = 2
PENALTY_SHARE = 0.4
LANES = 128
SUBLANES = 8
SPAN = 1
GROUP = 16
CHUNK = 32
PARTS = True
SMALL_LIMIT = 12 * 2**20

highest = lax.Precision.HIGHEST
f32 = jnp.float32
bf16 = jnp.bfloat16


def round_up(value, step):
    return -(-value // step) * step


def roll_rows(x, shift):
    return pltpu.roll(x, shift % x.shape[0], 0)


def row_pattern(stations):
    rows = lax.broadcasted_iota(jnp.int32, (SUBLANES, stations), 0)
    even = rows % 2 == 0
    first = rows % 4 < 2
    return even, first


def split_rows(x, even):
    high = x.astype(bf16).astype(f32)
    return jnp.where(even, high, x - high)


def add_pairs(x, even):
    return x + jnp.where(even, roll_rows(x, -1), roll_rows(x, 1))


def weigh_rows(load_square, magnitude):
    stations = magnitude.shape[1]
    column = magnitude.T[:, 0:1]
    total = jnp.zeros((SUBLANES, stations), f32)
    for r in range(stations // SUBLANES):
        part = slice(r * SUBLANES, (r + 1) * SUBLANES)
        total = total + load_square(r * SUBLANES, SUBLANES) * column[part]
    for shift in (4, 2, 1):
        total = total + roll_rows(total, shift)
    return total


def products(load_oper, load_square, load_parts, gain, even, first):
    stations = gain.shape[1]
    halves = split_rows(gain, even)
    crossed = roll_rows(halves, 2)
    crossed = jnp.where(first, -crossed, crossed).astype(bf16)
    halves = halves.astype(bf16)
    lhs = jnp.concatenate([halves, halves, crossed, crossed], axis=1)
    numerator = jnp.dot(lhs, load_oper(0, 4 * stations), preferred_element_type=f32)
    square = gain * gain
    magnitude = square + roll_rows(square, 2)
    if load_parts is None:
        denominator = weigh_rows(load_square, magnitude)
    else:
        lhs = split_rows(magnitude, even).astype(bf16)
        lhs = jnp.concatenate([lhs, lhs], axis=1)
        denominator = jnp.dot(
            lhs, load_parts(0, 2 * stations), preferred_element_type=f32
        )
        denominator = add_pairs(denominator, even)
    return add_pairs(numerator, even), denominator


def update(sums, gain, target_term, pen, average):
    numerator, denominator = sums
    updated = (numerator + target_term) / (denominator + pen)
    return 0.5 * (updated + gain) if average else updated


def to_rows(real, imag, first):
    return jnp.where(first, real, imag)


def band_weight(flags_ref, f, blocks):
    flagged = jnp.int32(0)
    for i in range(blocks):
        for j in range(blocks):
            flagged = flagged + flags_ref[f, i, j]
    kept = (blocks * blocks - flagged).astype(f32)
    return (1.0 + kept) / (1.0 + blocks * blocks)


def turn_steps(vis_ref, sky_ref, mask_ref, turned_ref):
    stations = mask_ref.shape[-1]
    width = LANES

    def turn_sky(a, c):
        part = pl.ds(c * width, width)
        turned_ref[a, part, :] = (sky_ref[a, :, part] * mask_ref[:, part]).T

    def turn_vis(a, c):
        part = pl.ds(c * width, width)
        turned_ref[2 + a, part, :] = vis_ref[a, :, part].T

    return [
        functools.partial(turn, a, c)
        for c in range(stations // width)
        for turn in (turn_sky, turn_vis)
        for a in range(2)
    ]


def combine_steps(turned_ref, oper_ref, square_ref, parts_ref, pen, first, pair, result):
    stations = turned_ref.shape[-1]
    chunk = CHUNK
    totals = [jnp.zeros((SUBLANES, stations), f32) for _ in range(3)]

    def combine(c):
        part = pl.ds(c * chunk, chunk)
        model_re, model_im, data_re, data_im = [
            turned_ref[a, part, :].astype(f32) for a in range(4)
        ]
        values = (
            model_re * data_re + model_im * data_im,
            model_re * data_im - model_im * data_re,
            model_re * model_re + model_im * model_im,
        )
        for n, value in enumerate(values):
            if n == 2:
                square_ref[pair, part, :] = value
            if n < 2 or PARTS:
                high = value.astype(bf16)
                low = (value - high.astype(f32)).astype(bf16)
                target = oper_ref.at[pair] if n < 2 else parts_ref
                start = (2 * n * stations if n < 2 else 0) + c * chunk
                target[pl.ds(start, chunk), :] = high
                target[pl.ds(start + stations, chunk), :] = low
            for r in range(chunk // SUBLANES):
                totals[n] = totals[n] + value[r * SUBLANES : (r + 1) * SUBLANES]

    def finish():
        sums = [jnp.sum(t, axis=0, keepdims=True) for t in totals]
        scale = sums[2] + pen
        result[pair] = to_rows((sums[0] + pen) / scale, sums[1] / scale, first)

    return [functools.partial(combine, c) for c in range(stations // chunk)] + [finish]


def merged(main, side):
    steps = []
    done = 0
    for n, step in enumerate(main):
        until = len(side) * (n + 1) // len(main)
        steps.append(step)
        steps += side[done:until]
        done = until
    return steps + side[done:]


def load_pair(ref, pair):
    return lambda start, size: ref[pair, pl.ds(start, size), :]


def first_kernel(
    flags_hbm, dest_hbm, vis_ref, sky_ref, oper_ref, square_ref, gain_ref,
    vis_buf, sky_buf, mask_ref, turned_ref, parts_ref, flags_ref, dest_ref, vis_sem, sky_sem, small_sem,
):
    bands, dirs, _, stations, _ = vis_ref.shape
    blocks = flags_ref.shape[-1]
    block = stations // blocks
    lanes = gain_ref.shape[1] - LANES
    even, first = row_pattern(stations)
    copies = []
    for k in range(dirs):
        copies.append(
            [
                pltpu.make_async_copy(source.at[:, k], buf.at[:, k], sem.at[k])
                for source, buf, sem in (
                    (sky_ref, sky_buf, sky_sem),
                    (vis_ref, vis_buf, vis_sem),
                )
            ]
        )
    ahead = 4
    for k in range(min(ahead, dirs)):
        for copy in copies[k]:
            copy.start()
    small = [
        pltpu.make_async_copy(flags_hbm, flags_ref, small_sem.at[0]),
        pltpu.make_async_copy(dest_hbm, dest_ref, small_sem.at[1]),
    ]
    for copy in small:
        copy.start()
    for copy in small:
        copy.wait()
    cols = lax.broadcasted_iota(jnp.int32, (block, stations), 1)
    rows = lax.broadcasted_iota(jnp.int32, (block, stations), 0)
    lane = lax.broadcasted_iota(jnp.int32, (1, LANES), 1)
    penalties = []
    for f in range(bands):
        for i in range(blocks):
            keep = jnp.zeros((block, stations), f32)
            for j in range(blocks):
                value = (1 - flags_ref[f, i, j]).astype(f32)
                keep = jnp.where(cols // block == j, value, keep)
            keep = jnp.where(cols == rows + i * block, 0.0, keep)
            mask_ref[f, pl.ds(i * block, block), :] = keep.astype(bf16)
        weight = band_weight(flags_ref, f, blocks)
        penalties.append(PENALTY_SHARE * stations * weight)
        extra = jnp.where(lane == 0, weight, dest_ref[f].astype(f32))
        extra = jnp.where(lane == 2, (lax.axis_index("band") * bands + f).astype(f32), extra)
        gain_ref[pl.ds(f, 1), pl.ds(lanes, LANES)] = extra
    gains = {}

    def sweep_step(pair, index):
        pen = penalties[pair % bands]
        sums = products(
            load_pair(oper_ref, pair),
            load_pair(square_ref, pair),
            load_pair(parts_ref, pair % parts_ref.shape[0]) if PARTS else None,
            gains[pair], even, first,
        )
        gains[pair] = update(
            sums, gains[pair], jnp.where(first, pen, 0.0), pen, index % 2 == 1
        )

    def slot(pair):
        return turned_ref.at[pair % turned_ref.shape[0]]

    def arrive(k):
        for copy in copies[k]:
            copy.wait()
        if k + ahead < dirs:
            for copy in copies[k + ahead]:
                copy.start()

    def turning(pair):
        k, f = divmod(pair, bands)
        steps = turn_steps(vis_buf.at[f, k], sky_buf.at[f, k], mask_ref.at[f], slot(pair))
        return [functools.partial(arrive, k)] * (f == 0) + steps

    def build_set(members):
        steps = [] if members[0] else turning(0)
        for pair in [k * bands + f for k in members for f in range(bands)]:
            combine = combine_steps(
                slot(pair), oper_ref, square_ref, parts_ref.at[pair % parts_ref.shape[0]],
                penalties[pair % bands], first, pair, gains
            )
            steps += merged(combine, turning(pair + 1) if pair + 1 < bands * dirs else [])
        return steps

    def sweep_set(members):
        pairs = [k * bands + f for k in members for f in range(bands)]
        return [
            functools.partial(sweep_step, p, index)
            for index in range(1, SWEEPS)
            for p in pairs
        ]

    sets = [list(range(k, min(k + SPAN, dirs))) for k in range(0, dirs, SPAN)]
    for n in range(len(sets) + 1):
        side = build_set(sets[n]) if n < len(sets) else []
        main = sweep_set(sets[n - 1]) if n else []
        for step in merged(main, side) if main else side:
            step()
        for k in sets[n - 1] if n else ():
            for f in range(bands):
                for a in range(2):
                    gain_ref[pl.ds(f, 1), pl.ds((k * 2 + a) * stations, stations)] = gains[
                        k * bands + f
                    ][2 * a : 2 * a + 1]


def chebyshev_columns(abscissa, width):
    lane = lax.broadcasted_iota(jnp.int32, (abscissa.shape[0], width), 1)
    terms = [jnp.ones_like(abscissa), abscissa]
    for degree in range(2, DEGREE + 1):
        terms.append(2.0 * abscissa * terms[-1] - terms[-2])
    basis = jnp.zeros((abscissa.shape[0], width), f32)
    for degree in range(DEGREE + 1):
        basis = jnp.where(lane == degree, terms[degree], basis)
    return basis


def fit_matrix(basis, weight):
    rows, width = basis.shape
    terms = round_up(DEGREE + 1, SUBLANES)
    span = round_up(rows, LANES)
    lane = lax.broadcasted_iota(jnp.int32, (rows, span), 1)
    row = lax.broadcasted_iota(jnp.int32, (rows, span), 0)
    identity = jnp.where(lane == row, 1.0, 0.0)
    weighted = basis * weight
    right = jnp.concatenate([basis, identity], axis=1)
    system = lax.dot_general(
        weighted, right, (((0,), (0,)), ((), ())), precision=highest,
        preferred_element_type=f32,
    )[:terms]
    line = lax.broadcasted_iota(jnp.int32, system.shape, 0)
    for j in range(DEGREE + 1):
        pivot = system[j : j + 1] / system[j : j + 1, j : j + 1]
        system = jnp.where(line == j, pivot, system - system[:, j : j + 1] * pivot)
    return system[:, width : width + rows], system[0:1, 0:1]


def assemble(pieces, all_ref):
    start = 0
    for piece in pieces:
        all_ref[pl.ds(start, piece.shape[0]), :] = piece[...]
        start += piece.shape[0]


def second_kernel(
    count, oper_ref, square_ref, *refs
):
    gain_ref, fresh_ref, dual_ref, fit_ref, extra_ref, all_ref = refs[count:]
    assemble(refs[:count], all_ref)
    bands = gain_ref.shape[0]
    lanes = gain_ref.shape[1]
    rows = all_ref.shape[0]
    pairs = oper_ref.shape[0]
    stations = oper_ref.shape[2]
    even, first = row_pattern(stations)
    basis = gathered_basis(all_ref[:, pl.ds(lanes, LANES)])
    weight = all_ref[:, pl.ds(lanes, 1)]
    extra_ref[...] = all_ref[:, pl.ds(lanes, LANES)]
    fit, _ = fit_matrix(basis, weight)
    fit_ref[...] = jnp.zeros_like(fit_ref)
    fit_ref[:, pl.ds(0, rows)] = fit
    project = jnp.dot(
        basis[:, : fit.shape[0]], fit, precision=highest, preferred_element_type=f32
    )
    own = all_ref[:, pl.ds(0, lanes)]
    fresh = jnp.dot(project, own, precision=highest, preferred_element_type=f32)
    fresh_ref[...] = fresh
    dual_ref[...] = own - fresh
    group = min(GROUP, pairs)
    for start in range(0, pairs, group):
        gains = []
        targets = []
        penalties = []
        for pair in range(start, start + group):
            k, f = divmod(pair, bands)
            pen = PENALTY_SHARE * stations * all_ref[pl.ds(f, 1), pl.ds(lanes, 1)]
            parts = [pl.ds((2 * k + a) * stations, stations) for a in range(2)]
            line = pl.ds(f, 1)
            gains.append(
                to_rows(all_ref[line, parts[0]], all_ref[line, parts[1]], first)
            )
            goal = [fresh_ref[line, p] - dual_ref[line, p] for p in parts]
            targets.append(pen * to_rows(goal[0], goal[1], first))
            penalties.append(pen)
        for index in range(SWEEPS):
            for n in range(group):
                sums = products(
                    load_pair(oper_ref, start + n), load_pair(square_ref, start + n), None,
                    gains[n], even, first,
                )
                gains[n] = update(sums, gains[n], targets[n], penalties[n], index % 2 == 1)
        for n in range(group):
            k, f = divmod(start + n, bands)
            for a in range(2):
                gain_ref[pl.ds(f, 1), pl.ds((2 * k + a) * stations, stations)] = gains[n][
                    2 * a : 2 * a + 1
                ]


def gathered_basis(extra):
    abscissa = (2.0 * extra[:, 2:3] + 1.0) / extra.shape[0] - 1.0
    return chebyshev_columns(abscissa, LANES)


def third_kernel(count, extra_ref, fresh_ref, dual_ref, fit_ref, *refs):
    delivered_ref, coefficients_ref, norm_ref, last_ref = refs[count:]
    assemble(refs[:count], last_ref)
    bands, dirs, _, stations = delivered_ref.shape
    rows, lanes = last_ref.shape
    extra = extra_ref[...]
    basis = gathered_basis(extra)
    weight, destination = extra[:, 0:1], extra[:, 1:2]
    fit = fit_ref[:, pl.ds(0, rows)]
    terms = fit.shape[0]
    gains = last_ref[...]
    dual = dual_ref[...]
    before = fresh_ref[...]
    coefficients = jnp.dot(
        fit, gains + dual, precision=highest, preferred_element_type=f32
    )
    fresh = jnp.dot(
        basis[:, :terms], coefficients, precision=highest, preferred_element_type=f32
    )
    line = lax.broadcasted_iota(jnp.int32, (rows, lanes), 1)
    start = jnp.where((line // stations) % 2 == 0, 1.0, 0.0)
    pieces = [dual * dual, (before - start) ** 2, (gains - fresh) ** 2, (fresh - before) ** 2]
    lane = lax.broadcasted_iota(jnp.int32, norm_ref.shape, 1)
    line = lax.broadcasted_iota(jnp.int32, norm_ref.shape, 0)
    norms = jnp.zeros(norm_ref.shape, f32)
    for n, piece in enumerate(pieces):
        here = (line == n // 2) & (lane == n % 2)
        norms = jnp.where(here, jnp.sum(piece * weight), norms)
    size = lax.axis_size("dir") * lanes
    norm_ref[...] = norms / (size * jnp.sum(weight))
    for k in range(dirs):
        for a in range(2):
            part = slice((2 * k + a) * stations, (2 * k + a + 1) * stations)
            for c in range(DEGREE + 1):
                coefficients_ref[c, k, pl.ds(a, 1), :] = coefficients[c : c + 1, part]
    for f in range(bands):
        target = extra[f : f + 1, 2:3]
        chosen = jnp.sum(jnp.where(destination == target, gains, 0.0), axis=0, keepdims=True)
        for k in range(dirs):
            for a in range(2):
                part = slice((2 * k + a) * stations, (2 * k + a + 1) * stations)
                delivered_ref[f, k, pl.ds(a, 1), :] = chosen[:, part]


def exchange(x, axis, distance):
    size = lax.axis_size(axis)
    return lax.ppermute(x, axis, [(i ^ distance, i) for i in range(size)])


def gather_rows(x, axis):
    size = lax.axis_size(axis)
    assert size & (size - 1) == 0
    distances = [2**n for n in range(size.bit_length() - 1)]
    for distance in distances[1:-1]:
        x = jnp.concatenate([x, exchange(x, axis, distance)], axis=0)
    if len(distances) == 1:
        return [x, exchange(x, axis, distances[0])]
    if len(distances) > 1:
        far = exchange(x, axis, distances[-1])
        near = exchange(x, axis, distances[0])
        return [x, near, far, exchange(far, axis, distances[0])]
    return [x]


def add_over(x, axis):
    size = lax.axis_size(axis)
    distance = 1
    while distance < size:
        x = x + exchange(x, axis, distance)
        distance *= 2
    return x


def vmem(*_):
    return pl.BlockSpec(memory_space=pltpu.VMEM)


def in_hbm(x):
    return pltpu.with_memory_space_constraint(x, pltpu.HBM)


def smem():
    return pl.BlockSpec(memory_space=pltpu.SMEM)


def per_device(visibilities, sky_model, rfi_flags, destination):
    bands, dirs, _, stations, _ = visibilities.shape
    count = lax.axis_size("band")
    rows = bands * count
    lanes = dirs * 2 * stations
    pairs = bands * dirs
    terms = round_up(DEGREE + 1, SUBLANES)
    hbm = pl.BlockSpec(memory_space=pltpu.HBM)
    operator, square, gains = pl.pallas_call(
        first_kernel,
        out_shape=(
            pltpu.VMEM((pairs, 4 * stations, stations), bf16),
            pltpu.VMEM((pairs, stations, stations), f32),
            jax.ShapeDtypeStruct((bands, lanes + LANES), f32),
        ),
        in_specs=[hbm, hbm, hbm, hbm],
        out_specs=(vmem(), vmem(), vmem()),
        scratch_shapes=[
            pltpu.VMEM((bands, dirs, 2, stations, stations), bf16),
            pltpu.VMEM((bands, dirs, 2, stations, stations), bf16),
            pltpu.VMEM((bands, stations, stations), bf16),
            pltpu.VMEM((2 * SPAN * bands, 4, stations, stations), bf16),
            pltpu.VMEM((2 * SPAN * bands, 2 * stations, stations), bf16),
            pltpu.SMEM(rfi_flags.shape, jnp.int32),
            pltpu.SMEM(destination.shape, jnp.int32),
            pltpu.SemaphoreType.DMA((dirs,)),
            pltpu.SemaphoreType.DMA((dirs,)),
            pltpu.SemaphoreType.DMA((2,)),
        ],
        compiler_params=pltpu.CompilerParams(vmem_limit_bytes=28 * 2**20),
        name="first",
    )(in_hbm(rfi_flags), in_hbm(destination), in_hbm(visibilities), in_hbm(sky_model))
    operator, square = [
        pltpu.with_memory_space_constraint(x, pltpu.VMEM) for x in (operator, square)
    ]
    pieces = gather_rows(gains, "band")
    gains, fresh, dual, fit, extra = pl.pallas_call(
        functools.partial(second_kernel, len(pieces)),
        out_shape=(
            pltpu.VMEM((bands, lanes), f32),
            pltpu.VMEM((rows, lanes), f32),
            pltpu.VMEM((rows, lanes), f32),
            pltpu.VMEM((terms, round_up(rows, LANES)), f32),
            pltpu.VMEM((rows, LANES), f32),
        ),
        in_specs=[vmem()] * (2 + len(pieces)),
        out_specs=(vmem(),) * 5,
        scratch_shapes=[pltpu.VMEM((rows, lanes + LANES), f32)],
        compiler_params=pltpu.CompilerParams(vmem_limit_bytes=SMALL_LIMIT),
        name="second",
    )(operator, square, *pieces)
    pieces = gather_rows(gains, "band")
    delivered, coefficients, norms = pl.pallas_call(
        functools.partial(third_kernel, len(pieces)),
        out_shape=(
            pltpu.VMEM((bands, dirs, 2, stations), f32),
            pltpu.VMEM((DEGREE + 1, dirs, 2, stations), f32),
            pltpu.VMEM((ITERS, LANES), f32),
        ),
        in_specs=[vmem()] * (4 + len(pieces)),
        out_specs=(vmem(),) * 3,
        scratch_shapes=[pltpu.VMEM((rows, lanes), f32)],
        compiler_params=pltpu.CompilerParams(vmem_limit_bytes=SMALL_LIMIT),
        name="third",
    )(extra, fresh, dual, fit, *pieces)
    norm_values = jnp.sqrt(add_over(norms, "dir")[:, :2])
    return delivered, coefficients, norm_values


def solution(mesh):
    return jax.shard_map(
        per_device,
        mesh=mesh,
        in_specs=(
            P("band", "dir", None, None, None),
            P("band", "dir", None, None, None),
            P("band", None, None),
            P("band"),
        ),
        out_specs=(P("band", "dir", None, None), P(None, "dir", None, None), P()),
        check_vma=False,
    )
```

```python
import functools

import jax
import jax.numpy as jnp
from jax import lax
from jax.experimental import pallas as pl
from jax.experimental.pallas import tpu as pltpu
from jax.sharding import PartitionSpec as P

DEGREE = 8
SWEEPS = 4
ITERS = 2
PENALTY_SHARE = 0.4
LANES = 128
SUBLANES = 8
SPAN = 1
GROUP = 16
CHUNK = 32
PARTS = True
AHEAD_FLOPS = 2 * 10**8
SMALL_LIMIT = 12 * 2**20

highest = lax.Precision.HIGHEST
f32 = jnp.float32
bf16 = jnp.bfloat16


def round_up(value, step):
    return -(-value // step) * step


def roll_rows(x, shift):
    return pltpu.roll(x, shift % x.shape[0], 0)


def row_pattern(stations):
    rows = lax.broadcasted_iota(jnp.int32, (SUBLANES, stations), 0)
    even = rows % 2 == 0
    first = rows % 4 < 2
    return even, first


def split_rows(x, even):
    high = x.astype(bf16).astype(f32)
    return jnp.where(even, high, x - high)


def add_pairs(x, even):
    return x + jnp.where(even, roll_rows(x, -1), roll_rows(x, 1))


def weigh_rows(load_square, magnitude):
    stations = magnitude.shape[1]
    column = magnitude.T[:, 0:1]
    total = jnp.zeros((SUBLANES, stations), f32)
    for r in range(stations // SUBLANES):
        part = slice(r * SUBLANES, (r + 1) * SUBLANES)
        total = total + load_square(r * SUBLANES, SUBLANES) * column[part]
    for shift in (4, 2, 1):
        total = total + roll_rows(total, shift)
    return total


def products(load_oper, load_square, load_parts, gain, even, first):
    stations = gain.shape[1]
    halves = split_rows(gain, even)
    crossed = roll_rows(halves, 2)
    crossed = jnp.where(first, -crossed, crossed).astype(bf16)
    halves = halves.astype(bf16)
    lhs = jnp.concatenate([halves, halves, crossed, crossed], axis=1)
    numerator = jnp.dot(lhs, load_oper(0, 4 * stations), preferred_element_type=f32)
    square = gain * gain
    magnitude = square + roll_rows(square, 2)
    if load_parts is None:
        denominator = weigh_rows(load_square, magnitude)
    else:
        lhs = split_rows(magnitude, even).astype(bf16)
        lhs = jnp.concatenate([lhs, lhs], axis=1)
        denominator = jnp.dot(
            lhs, load_parts(0, 2 * stations), preferred_element_type=f32
        )
        denominator = add_pairs(denominator, even)
    return add_pairs(numerator, even), denominator


def update(sums, gain, target_term, pen, average):
    numerator, denominator = sums
    updated = (numerator + target_term) / (denominator + pen)
    return 0.5 * (updated + gain) if average else updated


def to_rows(real, imag, first):
    return jnp.where(first, real, imag)


def band_weight(flags_ref, f, blocks):
    flagged = jnp.int32(0)
    for i in range(blocks):
        for j in range(blocks):
            flagged = flagged + flags_ref[f, i, j]
    kept = (blocks * blocks - flagged).astype(f32)
    return (1.0 + kept) / (1.0 + blocks * blocks)


def turn_steps(vis_ref, sky_ref, mask_ref, turned_ref):
    stations = mask_ref.shape[-1]
    width = LANES

    def turn_sky(a, c):
        part = pl.ds(c * width, width)
        turned_ref[a, part, :] = (sky_ref[a, :, part] * mask_ref[:, part]).T

    def turn_vis(a, c):
        part = pl.ds(c * width, width)
        turned_ref[2 + a, part, :] = vis_ref[a, :, part].T

    return [
        functools.partial(turn, a, c)
        for c in range(stations // width)
        for turn in (turn_sky, turn_vis)
        for a in range(2)
    ]


def combine_steps(turned_ref, oper_ref, square_ref, parts_ref, pen, first, pair, result):
    stations = turned_ref.shape[-1]
    chunk = CHUNK
    totals = [jnp.zeros((SUBLANES, stations), f32) for _ in range(3)]

    def combine(c):
        part = pl.ds(c * chunk, chunk)
        model_re, model_im, data_re, data_im = [
            turned_ref[a, part, :].astype(f32) for a in range(4)
        ]
        values = (
            model_re * data_re + model_im * data_im,
            model_re * data_im - model_im * data_re,
            model_re * model_re + model_im * model_im,
        )
        for n, value in enumerate(values):
            if n == 2:
                square_ref[pair, part, :] = value
            if n < 2 or PARTS:
                high = value.astype(bf16)
                low = (value - high.astype(f32)).astype(bf16)
                target = oper_ref.at[pair] if n < 2 else parts_ref
                start = (2 * n * stations if n < 2 else 0) + c * chunk
                target[pl.ds(start, chunk), :] = high
                target[pl.ds(start + stations, chunk), :] = low
            for r in range(chunk // SUBLANES):
                totals[n] = totals[n] + value[r * SUBLANES : (r + 1) * SUBLANES]

    def finish():
        sums = [jnp.sum(t, axis=0, keepdims=True) for t in totals]
        scale = sums[2] + pen
        result[pair] = to_rows((sums[0] + pen) / scale, sums[1] / scale, first)

    return [functools.partial(combine, c) for c in range(stations // chunk)] + [finish]


def merged(main, side):
    steps = []
    done = 0
    for n, step in enumerate(main):
        until = len(side) * (n + 1) // len(main)
        steps.append(step)
        steps += side[done:until]
        done = until
    return steps + side[done:]


def load_pair(ref, pair):
    return lambda start, size: ref[pair, pl.ds(start, size), :]


def first_kernel(
    flags_hbm, dest_hbm, vis_ref, sky_ref, oper_ref, square_ref, gain_ref,
    vis_buf, sky_buf, mask_ref, turned_ref, parts_ref, flags_ref, dest_ref, vis_sem, sky_sem, small_sem,
):
    bands, dirs, _, stations, _ = vis_ref.shape
    blocks = flags_ref.shape[-1]
    block = stations // blocks
    lanes = gain_ref.shape[1] - LANES
    even, first = row_pattern(stations)
    copies = []
    for k in range(dirs):
        copies.append(
            [
                pltpu.make_async_copy(source.at[:, k], buf.at[:, k], sem.at[k])
                for source, buf, sem in (
                    (sky_ref, sky_buf, sky_sem),
                    (vis_ref, vis_buf, vis_sem),
                )
            ]
        )
    small = [
        pltpu.make_async_copy(flags_hbm, flags_ref, small_sem.at[0]),
        pltpu.make_async_copy(dest_hbm, dest_ref, small_sem.at[1]),
    ]
    for copy in small:
        copy.start()
    ahead = 2
    for k in range(min(ahead, dirs)):
        for copy in copies[k]:
            copy.start()
    for copy in small:
        copy.wait()
    cols = lax.broadcasted_iota(jnp.int32, (block, stations), 1)
    rows = lax.broadcasted_iota(jnp.int32, (block, stations), 0)
    lane = lax.broadcasted_iota(jnp.int32, (1, LANES), 1)
    penalties = []
    for f in range(bands):
        for i in range(blocks):
            keep = jnp.zeros((block, stations), f32)
            for j in range(blocks):
                value = (1 - flags_ref[f, i, j]).astype(f32)
                keep = jnp.where(cols // block == j, value, keep)
            keep = jnp.where(cols == rows + i * block, 0.0, keep)
            mask_ref[f, pl.ds(i * block, block), :] = keep.astype(bf16)
        weight = band_weight(flags_ref, f, blocks)
        penalties.append(PENALTY_SHARE * stations * weight)
        extra = jnp.where(lane == 0, weight, dest_ref[f].astype(f32))
        extra = jnp.where(lane == 2, (lax.axis_index("band") * bands + f).astype(f32), extra)
        gain_ref[pl.ds(f, 1), pl.ds(lanes, LANES)] = extra
    gains = {}

    def sweep_step(pair, index):
        pen = penalties[pair % bands]
        sums = products(
            load_pair(oper_ref, pair),
            load_pair(square_ref, pair),
            load_pair(parts_ref, pair % parts_ref.shape[0]) if PARTS else None,
            gains[pair], even, first,
        )
        gains[pair] = update(
            sums, gains[pair], jnp.where(first, pen, 0.0), pen, index % 2 == 1
        )

    def slot(pair):
        return turned_ref.at[pair % turned_ref.shape[0]]

    def arrive(k):
        for copy in copies[k]:
            copy.wait()
        if k + ahead < dirs:
            for copy in copies[k + ahead]:
                copy.start()

    def turning(pair):
        k, f = divmod(pair, bands)
        steps = turn_steps(vis_buf.at[f, k], sky_buf.at[f, k], mask_ref.at[f], slot(pair))
        return [functools.partial(arrive, k)] * (f == 0) + steps

    def build_set(members):
        steps = [] if members[0] else turning(0)
        for pair in [k * bands + f for k in members for f in range(bands)]:
            combine = combine_steps(
                slot(pair), oper_ref, square_ref, parts_ref.at[pair % parts_ref.shape[0]],
                penalties[pair % bands], first, pair, gains
            )
            steps += merged(combine, turning(pair + 1) if pair + 1 < bands * dirs else [])
        return steps

    def sweep_set(members):
        pairs = [k * bands + f for k in members for f in range(bands)]
        return [
            functools.partial(sweep_step, p, index)
            for index in range(1, SWEEPS)
            for p in pairs
        ]

    sets = [list(range(k, min(k + SPAN, dirs))) for k in range(0, dirs, SPAN)]
    for n in range(len(sets) + 1):
        side = build_set(sets[n]) if n < len(sets) else []
        main = sweep_set(sets[n - 1]) if n else []
        for step in merged(main, side) if main else side:
            step()
        for k in sets[n - 1] if n else ():
            for f in range(bands):
                for a in range(2):
                    gain_ref[pl.ds(f, 1), pl.ds((k * 2 + a) * stations, stations)] = gains[
                        k * bands + f
                    ][2 * a : 2 * a + 1]


def load_gain(gain_ref, pair, bands, stations, first):
    k, f = divmod(pair, bands)
    real, imag = [
        gain_ref[pl.ds(f, 1), pl.ds((2 * k + a) * stations, stations)] for a in range(2)
    ]
    return to_rows(real, imag, first)


def ahead_kernel(oper_ref, square_ref, gain_ref, numerator_ref, denominator_ref):
    bands = gain_ref.shape[0]
    pairs, stations, _ = square_ref.shape
    even, first = row_pattern(stations)
    for pair in range(pairs):
        numerator_ref[pair], denominator_ref[pair] = products(
            load_pair(oper_ref, pair), load_pair(square_ref, pair), None,
            load_gain(gain_ref, pair, bands, stations, first), even, first,
        )


def chebyshev_columns(abscissa, width):
    lane = lax.broadcasted_iota(jnp.int32, (abscissa.shape[0], width), 1)
    terms = [jnp.ones_like(abscissa), abscissa]
    for degree in range(2, DEGREE + 1):
        terms.append(2.0 * abscissa * terms[-1] - terms[-2])
    basis = jnp.zeros((abscissa.shape[0], width), f32)
    for degree in range(DEGREE + 1):
        basis = jnp.where(lane == degree, terms[degree], basis)
    return basis


def fit_matrix(basis, weight):
    rows, width = basis.shape
    terms = round_up(DEGREE + 1, SUBLANES)
    span = round_up(rows, LANES)
    lane = lax.broadcasted_iota(jnp.int32, (rows, span), 1)
    row = lax.broadcasted_iota(jnp.int32, (rows, span), 0)
    identity = jnp.where(lane == row, 1.0, 0.0)
    weighted = basis * weight
    right = jnp.concatenate([basis, identity], axis=1)
    system = lax.dot_general(
        weighted, right, (((0,), (0,)), ((), ())), precision=highest,
        preferred_element_type=f32,
    )[:terms]
    line = lax.broadcasted_iota(jnp.int32, system.shape, 0)
    for j in range(DEGREE + 1):
        pivot = system[j : j + 1] / system[j : j + 1, j : j + 1]
        system = jnp.where(line == j, pivot, system - system[:, j : j + 1] * pivot)
    return system[:, width : width + rows], system[0:1, 0:1]


def assemble(pieces, all_ref):
    start = 0
    for piece in pieces:
        all_ref[pl.ds(start, piece.shape[0]), :] = piece[...]
        start += piece.shape[0]


def second_kernel(count, oper_ref, square_ref, numerator_ref, denominator_ref, *refs):
    gain_ref, fresh_ref, dual_ref, fit_ref, extra_ref, all_ref = refs[count:]
    assemble(refs[:count], all_ref)
    bands = gain_ref.shape[0]
    lanes = gain_ref.shape[1]
    rows = all_ref.shape[0]
    pairs = oper_ref.shape[0]
    stations = oper_ref.shape[2]
    even, first = row_pattern(stations)
    basis = gathered_basis(all_ref[:, pl.ds(lanes, LANES)])
    weight = all_ref[:, pl.ds(lanes, 1)]
    extra_ref[...] = all_ref[:, pl.ds(lanes, LANES)]
    fit, _ = fit_matrix(basis, weight)
    fit_ref[...] = jnp.zeros_like(fit_ref)
    fit_ref[:, pl.ds(0, rows)] = fit
    project = jnp.dot(
        basis[:, : fit.shape[0]], fit, precision=highest, preferred_element_type=f32
    )
    own = all_ref[:, pl.ds(0, lanes)]
    fresh = jnp.dot(project, own, precision=highest, preferred_element_type=f32)
    fresh_ref[...] = fresh
    dual_ref[...] = own - fresh
    group = min(GROUP, pairs)
    for start in range(0, pairs, group):
        gains = []
        targets = []
        penalties = []
        for pair in range(start, start + group):
            k, f = divmod(pair, bands)
            pen = PENALTY_SHARE * stations * all_ref[pl.ds(f, 1), pl.ds(lanes, 1)]
            parts = [pl.ds((2 * k + a) * stations, stations) for a in range(2)]
            line = pl.ds(f, 1)
            gains.append(load_gain(all_ref, pair, bands, stations, first))
            goal = [fresh_ref[line, p] - dual_ref[line, p] for p in parts]
            targets.append(pen * to_rows(goal[0], goal[1], first))
            penalties.append(pen)
        for index in range(SWEEPS):
            for n in range(group):
                if index == 0:
                    sums = numerator_ref[start + n], denominator_ref[start + n]
                else:
                    sums = products(
                        load_pair(oper_ref, start + n), load_pair(square_ref, start + n), None,
                        gains[n], even, first,
                    )
                gains[n] = update(sums, gains[n], targets[n], penalties[n], index % 2 == 1)
        for n in range(group):
            k, f = divmod(start + n, bands)
            for a in range(2):
                gain_ref[pl.ds(f, 1), pl.ds((2 * k + a) * stations, stations)] = gains[n][
                    2 * a : 2 * a + 1
                ]


def gathered_basis(extra):
    abscissa = (2.0 * extra[:, 2:3] + 1.0) / extra.shape[0] - 1.0
    return chebyshev_columns(abscissa, LANES)


def third_kernel(count, extra_ref, fresh_ref, dual_ref, fit_ref, *refs):
    delivered_ref, coefficients_ref, norm_ref, last_ref = refs[count:]
    assemble(refs[:count], last_ref)
    bands, dirs, _, stations = delivered_ref.shape
    rows, lanes = last_ref.shape
    extra = extra_ref[...]
    basis = gathered_basis(extra)
    weight, destination = extra[:, 0:1], extra[:, 1:2]
    fit = fit_ref[:, pl.ds(0, rows)]
    terms = fit.shape[0]
    gains = last_ref[...]
    dual = dual_ref[...]
    before = fresh_ref[...]
    coefficients = jnp.dot(
        fit, gains + dual, precision=highest, preferred_element_type=f32
    )
    fresh = jnp.dot(
        basis[:, :terms], coefficients, precision=highest, preferred_element_type=f32
    )
    line = lax.broadcasted_iota(jnp.int32, (rows, lanes), 1)
    start = jnp.where((line // stations) % 2 == 0, 1.0, 0.0)
    pieces = [dual * dual, (before - start) ** 2, (gains - fresh) ** 2, (fresh - before) ** 2]
    lane = lax.broadcasted_iota(jnp.int32, norm_ref.shape, 1)
    line = lax.broadcasted_iota(jnp.int32, norm_ref.shape, 0)
    norms = jnp.zeros(norm_ref.shape, f32)
    for n, piece in enumerate(pieces):
        here = (line == n // 2) & (lane == n % 2)
        norms = jnp.where(here, jnp.sum(piece * weight), norms)
    size = lax.axis_size("dir") * lanes
    norm_ref[...] = norms / (size * jnp.sum(weight))
    for k in range(dirs):
        for a in range(2):
            part = slice((2 * k + a) * stations, (2 * k + a + 1) * stations)
            for c in range(DEGREE + 1):
                coefficients_ref[c, k, pl.ds(a, 1), :] = coefficients[c : c + 1, part]
    for f in range(bands):
        target = extra[f : f + 1, 2:3]
        chosen = jnp.sum(jnp.where(destination == target, gains, 0.0), axis=0, keepdims=True)
        for k in range(dirs):
            for a in range(2):
                part = slice((2 * k + a) * stations, (2 * k + a + 1) * stations)
                delivered_ref[f, k, pl.ds(a, 1), :] = chosen[:, part]


def exchange(x, axis, distance):
    size = lax.axis_size(axis)
    return lax.ppermute(x, axis, [(i ^ distance, i) for i in range(size)])


def gather_rows(x, axis):
    size = lax.axis_size(axis)
    assert size & (size - 1) == 0
    distances = [2**n for n in range(size.bit_length() - 1)]
    for distance in distances[1:-1]:
        x = jnp.concatenate([x, exchange(x, axis, distance)], axis=0)
    if len(distances) == 1:
        return [x, exchange(x, axis, distances[0])]
    if len(distances) > 1:
        far = exchange(x, axis, distances[-1])
        near = exchange(x, axis, distances[0])
        return [x, near, far, exchange(far, axis, distances[0])]
    return [x]


def add_over(x, axis):
    size = lax.axis_size(axis)
    distance = 1
    while distance < size:
        x = x + exchange(x, axis, distance)
        distance *= 2
    return x


def vmem(*_):
    return pl.BlockSpec(memory_space=pltpu.VMEM)


def in_hbm(x):
    return pltpu.with_memory_space_constraint(x, pltpu.HBM)


def smem():
    return pl.BlockSpec(memory_space=pltpu.SMEM)


def per_device(visibilities, sky_model, rfi_flags, destination):
    bands, dirs, _, stations, _ = visibilities.shape
    count = lax.axis_size("band")
    rows = bands * count
    lanes = dirs * 2 * stations
    pairs = bands * dirs
    terms = round_up(DEGREE + 1, SUBLANES)
    hbm = pl.BlockSpec(memory_space=pltpu.HBM)
    operator, square, gains = pl.pallas_call(
        first_kernel,
        out_shape=(
            pltpu.VMEM((pairs, 4 * stations, stations), bf16),
            pltpu.VMEM((pairs, stations, stations), f32),
            jax.ShapeDtypeStruct((bands, lanes + LANES), f32),
        ),
        in_specs=[hbm, hbm, hbm, hbm],
        out_specs=(vmem(), vmem(), vmem()),
        scratch_shapes=[
            pltpu.VMEM((bands, dirs, 2, stations, stations), bf16),
            pltpu.VMEM((bands, dirs, 2, stations, stations), bf16),
            pltpu.VMEM((bands, stations, stations), bf16),
            pltpu.VMEM((2 * SPAN * bands, 4, stations, stations), bf16),
            pltpu.VMEM((2 * SPAN * bands, 2 * stations, stations), bf16),
            pltpu.SMEM(rfi_flags.shape, jnp.int32),
            pltpu.SMEM(destination.shape, jnp.int32),
            pltpu.SemaphoreType.DMA((dirs,)),
            pltpu.SemaphoreType.DMA((dirs,)),
            pltpu.SemaphoreType.DMA((2,)),
        ],
        compiler_params=pltpu.CompilerParams(vmem_limit_bytes=28 * 2**20),
        name="first",
    )(in_hbm(rfi_flags), in_hbm(destination), in_hbm(visibilities), in_hbm(sky_model))
    operator, square = [
        pltpu.with_memory_space_constraint(x, pltpu.VMEM) for x in (operator, square)
    ]
    pieces = gather_rows(gains, "band")
    sums = pl.pallas_call(
        ahead_kernel,
        out_shape=(pltpu.VMEM((pairs, SUBLANES, stations), f32),) * 2,
        in_specs=[vmem()] * 3,
        out_specs=(vmem(),) * 2,
        compiler_params=pltpu.CompilerParams(vmem_limit_bytes=SMALL_LIMIT),
        cost_estimate=pl.CostEstimate(
            flops=AHEAD_FLOPS, bytes_accessed=0, transcendentals=0
        ),
        name="ahead",
    )(operator, square, gains)
    gains, fresh, dual, fit, extra = pl.pallas_call(
        functools.partial(second_kernel, len(pieces)),
        out_shape=(
            pltpu.VMEM((bands, lanes), f32),
            pltpu.VMEM((rows, lanes), f32),
            pltpu.VMEM((rows, lanes), f32),
            pltpu.VMEM((terms, round_up(rows, LANES)), f32),
            pltpu.VMEM((rows, LANES), f32),
        ),
        in_specs=[vmem()] * (4 + len(pieces)),
        out_specs=(vmem(),) * 5,
        scratch_shapes=[pltpu.VMEM((rows, lanes + LANES), f32)],
        compiler_params=pltpu.CompilerParams(vmem_limit_bytes=SMALL_LIMIT),
        name="second",
    )(operator, square, *sums, *pieces)
    pieces = gather_rows(gains, "band")
    delivered, coefficients, norms = pl.pallas_call(
        functools.partial(third_kernel, len(pieces)),
        out_shape=(
            pltpu.VMEM((bands, dirs, 2, stations), f32),
            pltpu.VMEM((DEGREE + 1, dirs, 2, stations), f32),
            pltpu.VMEM((ITERS, LANES), f32),
        ),
        in_specs=[vmem()] * (4 + len(pieces)),
        out_specs=(vmem(),) * 3,
        scratch_shapes=[pltpu.VMEM((rows, lanes), f32)],
        compiler_params=pltpu.CompilerParams(vmem_limit_bytes=SMALL_LIMIT),
        name="third",
    )(extra, fresh, dual, fit, *pieces)
    norm_values = jnp.sqrt(add_over(norms, "dir")[:, :2])
    return delivered, coefficients, norm_values


def solution(mesh):
    return jax.shard_map(
        per_device,
        mesh=mesh,
        in_specs=(
            P("band", "dir", None, None, None),
            P("band", "dir", None, None, None),
            P("band", None, None),
            P("band"),
        ),
        out_specs=(P("band", "dir", None, None), P(None, "dir", None, None), P()),
        check_vma=False,
    )
```
